32 devices in a mesh: gx: 4 (over y, x), gy: 8 (over z, core).
Axes of the slice: x: 2, y: 2, z: 4, core: 2. Of those that a mesh axis runs over, the one named last changes fastest.
Arguments:
- schur_blocks: float32 [32, 2048, 2048], P(('gx', 'gy')), may hold values from -1 to 11, as said below
- offsets: int32 [32], P(('gx', 'gy')), may hold values from 256 to 768, as said below
- right_side: float32 [32768, 128], P(('gx', 'gy')), may hold values from -20 to 20
- coarse_basis: float32 [32768, 128], P(('gx', 'gy')), may hold values from -0.03125 to 0.03125
- coarse_load: float32 [128, 128], replicated, may hold values from -6 to 6
Outputs:
- multipliers: float32 [32768, 128], P(('gx', 'gy'))
- amplitudes: float32 [128, 128], replicated
The draws below stay inside these ranges and needn't reach their ends.
Inputs may be any that keep to these rules, and one draw needn't show every extreme that they name: `schur_blocks`: each block is symmetric positive definite. `offsets`: both ends of the range are taken by some subdomain.
All inputs are finite; a program needn't handle non-finite values.
Results may differ from the reference program's by a relative error of at most 0.0003.
Values sent between devices are 32-bit elements; how exact they have to be, the bound alone decides.
A program may use at most 128 MiB of HBM per device.

```python
import math
import jax
import jax.numpy as jnp
from jax import lax

W = 2048
SLAB = 1024
R = 128
NC = 128
ITERS = 3
SUBDOMAINS = 32
MULTS = 32768


def draw_schur_blocks(key, part):
    upper_end = 4.0
    subkeys = jax.random.split(key, SUBDOMAINS)

    def single(subkey):
        diag_key, noise_key = jax.random.split(subkey)
        diagonal = jnp.exp(jax.random.uniform(diag_key, (W,), jnp.float32, 0.0, math.log(upper_end)))
        noise_part = jax.random.truncated_normal(noise_key, -5.0, 5.0, (W, W), jnp.float32) * (0.25 / math.sqrt(W))
        return jnp.diag(diagonal) + (noise_part + noise_part.T) * 0.7071067811865476
    return lax.map(single, subkeys)


def draw_offsets(key, part):
    key_values, key_ranking = jax.random.split(key)
    lowest = SLAB // 4
    highest = 3 * SLAB // 4
    values = jax.random.randint(key_values, (SUBDOMAINS,), lowest, highest + 1).astype(jnp.int32)
    ranking = jax.random.permutation(key_ranking, SUBDOMAINS)
    values = values.at[ranking[0]].set(lowest).at[ranking[1]].set(highest)
    return values.astype(jnp.int32)


def draw_right_side(key, part):
    base_key = jax.random.fold_in(key, 0)
    total_rows = SLAB * SUBDOMAINS
    position = jnp.arange(total_rows, dtype=jnp.float32) / total_rows
    base = jax.random.truncated_normal(base_key, -4.0, 4.0, (total_rows, R), jnp.float32)
    rising = 1.0 + 2.0 * position
    return base * rising[:, None]


def block_scale(stream_key, dims, cuts, low, top_value):
    gain, own = 1.0, jax.random.fold_in(stream_key, 6)
    for dim, shards_of in cuts:
        heights = jnp.exp(jax.random.uniform(jax.random.fold_in(own, dim), (shards_of,), jnp.float32, low / len(cuts), top_value / len(cuts)))
        gain = gain * jnp.repeat(heights, dims[dim] // shards_of).reshape([-1 if axis == dim else 1 for axis in range(len(dims))])
    return gain


def gaussian(stream_key, extent, spread, reach, pieces=(), kind=jnp.bfloat16):
    values = jax.random.normal(stream_key, extent, jnp.float32) * spread
    if len(pieces) > 0:
        values = block_scale(stream_key, extent, pieces, -0.22, 0.18) * values
    return jnp.clip(values, min=-reach, max=reach).astype(kind)


def setup_inputs(seed: int = 0) -> dict:
    keys = jax.random.split(jax.random.key(seed), 6)
    return {
        "schur_blocks": draw_schur_blocks(jax.random.fold_in(keys[5], 71), 0),
        "offsets": draw_offsets(jax.random.fold_in(keys[5], 71), 0),
        "right_side": draw_right_side(jax.random.fold_in(keys[5], 71), 0),
        "coarse_basis": gaussian(keys[3], (MULTS, NC), MULTS ** -0.5, 0.03125, ((0, 32),), jnp.float32),
        "coarse_load": gaussian(keys[4], (NC, R), 1.0, 6.0, (), jnp.float32),
    }


HIGHEST = lax.Precision.HIGHEST

def apply_operator(vector, schur_blocks, offsets):
    padded = jnp.pad(vector, ((SLAB, SLAB), (0, 0)))

    def visit_block(accumulated, inputs):
        schur_block, start_row, device_index = inputs
        first_row = (device_index * SLAB + start_row).astype(jnp.int32)
        window = lax.dynamic_slice_in_dim(padded, first_row, W, 0)
        product_block = jnp.dot(schur_block.astype(jnp.float32), window.astype(jnp.float32), precision=HIGHEST, preferred_element_type=jnp.float32)
        current = lax.dynamic_slice_in_dim(accumulated, first_row, W, 0)
        return (lax.dynamic_update_slice_in_dim(accumulated, current + product_block, first_row, 0), None)
    indices = jnp.arange(SUBDOMAINS, dtype=jnp.int32)
    accumulated, _ = lax.scan(visit_block, jnp.zeros_like(padded), (schur_blocks, offsets.astype(jnp.int32), indices))
    return accumulated[SLAB:SLAB + vector.shape[0]]

def project(residual, coarse_basis, gram_factor):
    coarse_part = jnp.dot(coarse_basis.T.astype(jnp.float32), residual.astype(jnp.float32), precision=HIGHEST, preferred_element_type=jnp.float32)
    amplitudes = jax.scipy.linalg.cho_solve((gram_factor, True), coarse_part)
    projected = residual - jnp.dot(coarse_basis.astype(jnp.float32), amplitudes.astype(jnp.float32), precision=HIGHEST, preferred_element_type=jnp.float32)
    return (projected, amplitudes)

def reference(schur_blocks, offsets, right_side, coarse_basis, coarse_load):
    gram_matrix = jnp.dot(coarse_basis.T.astype(jnp.float32), coarse_basis.astype(jnp.float32), precision=HIGHEST, preferred_element_type=jnp.float32)
    gram_factor = jnp.linalg.cholesky(gram_matrix)
    start_load = jax.scipy.linalg.cho_solve((gram_factor, True), coarse_load)
    multipliers = jnp.dot(coarse_basis.astype(jnp.float32), start_load.astype(jnp.float32), precision=HIGHEST, preferred_element_type=jnp.float32)
    residual = right_side - apply_operator(multipliers, schur_blocks, offsets)
    projected, amplitudes = project(residual, coarse_basis, gram_factor)
    direction = projected
    energy_now = jnp.sum(projected * projected, axis=0)
    for iteration in range(ITERS):
        operator_image = apply_operator(direction, schur_blocks, offsets)
        step_length = energy_now / jnp.sum(direction * operator_image, axis=0)
        multipliers = multipliers + step_length * direction
        residual = residual - step_length * operator_image
        projected, amplitudes = project(residual, coarse_basis, gram_factor)
        energy_next = jnp.sum(projected * projected, axis=0)
        direction = projected + energy_next / energy_now * direction
        energy_now = energy_next
    return (multipliers, amplitudes)
```

```python
import functools

import jax
import jax.numpy as jnp
from jax import lax
from jax.experimental import pallas as pl
from jax.experimental.pallas import tpu as pltpu
from jax.sharding import PartitionSpec as P

ITERS = 3
MESH = pl.DeviceIdType.MESH
HIGHEST = lax.Precision.HIGHEST
F32 = jnp.float32
BF16 = jnp.bfloat16
LANES = 128
CHUNK = 128
SLOTS = 4
BLOCK = 512
EXCHANGES = 3 + 2 * (ITERS - 1)
PARTS = ITERS
IMAGES = ITERS
REDUCES = 2 + ITERS
STEPS = ((1,), (2,), (0, 3))


def dot(a, b):
    return jnp.dot(a, b, precision=HIGHEST, preferred_element_type=F32)


def halves(x):
    hi = x.astype(BF16)
    return hi, (x - hi.astype(F32)).astype(BF16)


def narrow(x):
    return jnp.concatenate(halves(x), axis=1)


def right_operand(x):
    hi, lo = halves(x)
    return jnp.concatenate(
        [jnp.concatenate([hi, lo], axis=1), jnp.concatenate([hi, jnp.zeros_like(lo)], axis=1)], axis=0
    )


def small(left, right):
    both = jnp.dot(left, right, preferred_element_type=F32)
    half = both.shape[1] // 2
    return both[:, :half] + both[:, half:]


def kernel(nx, ny, off_ref, schur_ref, right_hbm, basis_hbm, load_hbm, lam_hbm, amp_hbm, s):
    n = nx * ny
    slab, nc = s["right"].shape
    width = 2 * slab
    low = slab // 4
    span = slab - low
    ix, iy = lax.axis_index("gx"), lax.axis_index("gy")
    me = ix * ny + iy
    off = off_ref[0]
    chunks = width // CHUNK
    tiles = width // LANES
    stages = [s["stage%d" % i] for i in range(SLOTS)]
    s_hi, s_lo, vec, twice = s["s_hi"], s["s_lo"], s["vec"], s["twice"]
    in_l, in_r, out_l, out_r, img = s["in_l"], s["in_r"], s["out_l"], s["out_r"], s["img"]
    right, basis_own, load = s["right"], s["basis_own"], s["load"]
    basis_w, basis_hl, sc, sc_hl = s["basis_w"], s["basis_hl"], s["sc"], s["sc_hl"]
    p_ref, z, base, zbase, si = s["p"], s["z"], s["base"], s["zbase"], s["si"]
    lam, amp_out, d = s["lam"], s["amp"], s["d"]
    m_ref, sweep = s["m"], s["sweep"]
    scal_in, scal_mid, scal_x, scal_y = s["scal_in"], s["scal_mid"], s["scal_x"], s["scal_y"]

    def where_is(i):
        return (lax.div(i, ny), lax.rem(i, ny))

    def fetch(i, slot):
        return pltpu.make_async_copy(
            schur_ref.at[pl.ds(i * CHUNK, CHUNK), :], stages[slot], s["stage_sem"].at[slot]
        )

    def load_in(k):
        src, dst = ((basis_hbm, basis_own), (right_hbm, right), (load_hbm, load))[k]
        return pltpu.make_async_copy(src, dst, s["load_sem"].at[k])

    load_in(0).start()
    barrier = pltpu.get_barrier_semaphore()

    def greet(x, y):
        pl.semaphore_signal(barrier, inc=1, device_id=(x, y), device_id_type=MESH)

    def greet_x(k, carry):
        greet(lax.rem(ix + k, nx), iy)
        return carry

    def greet_y(k, carry):
        greet(ix, lax.rem(iy + k, ny))
        return carry

    turns_left = jnp.logical_and(iy == 0, ix > 0)
    turns_right = jnp.logical_and(iy == ny - 1, ix < nx - 1)

    lax.fori_loop(1, nx, greet_x, 0)
    lax.fori_loop(1, ny, greet_y, 0)

    @pl.when(turns_left)
    def _():
        greet(ix - 1, ny - 1)

    @pl.when(turns_right)
    def _():
        greet(ix + 1, 0)

    load_in(1).start()
    for i in range(SLOTS):
        fetch(i, i).start()
    load_in(2).start()

    @pl.when(me == 0)
    def _():
        in_l[...] = jnp.zeros_like(in_l)

    @pl.when(me == n - 1)
    def _():
        in_r[...] = jnp.zeros_like(in_r)

    def to_right(e, i, src):
        return pltpu.make_async_remote_copy(
            src_ref=src, dst_ref=in_l.at[e, pl.ds(i * low, low)], send_sem=s["hs_r"].at[e, i],
            recv_sem=s["hr_l"].at[e, i], device_id=where_is(lax.rem(me + 1, n)), device_id_type=MESH,
        )

    def to_left(e, i, src):
        return pltpu.make_async_remote_copy(
            src_ref=src, dst_ref=in_r.at[e, pl.ds(i * low, low)], send_sem=s["hs_l"].at[e, i],
            recv_sem=s["hr_r"].at[e, i], device_id=where_is(lax.rem(me + n - 1, n)), device_id_type=MESH,
        )

    any_part = out_l.at[0, pl.ds(0, low)]

    def send(e, i_right, src_right, i_left, src_left):
        if src_left is not None:
            @pl.when(me > 0)
            def _():
                to_left(e, i_left, src_left).start()

        if src_right is not None:
            @pl.when(me < n - 1)
            def _():
                to_right(e, i_right, src_right).start()

    def from_left(e, i):
        @pl.when(me > 0)
        def _():
            to_right(e, i, any_part).wait_recv()

        return in_l[e, i * low : (i + 1) * low, :]

    def from_right(e, i):
        @pl.when(me < n - 1)
        def _():
            to_left(e, i, any_part).wait_recv()

        return in_r[e, i * low : (i + 1) * low, :]

    def below(c):
        return lax.broadcasted_iota(jnp.int32, (low, nc), 0) + c * low < off

    def q(c):
        return slice(c * low, (c + 1) * low)

    def own_q(c):
        return slice(slab + c * low, slab + (c + 1) * low)

    def send_own(e, c, ref):
        view = ref.at[pl.ds(c * low, low)]
        send(e, c - 1, view if c > 0 else None, c, view if c < 3 else None)

    def halo(e, c):
        if c == 0:
            return from_right(e, 0)
        if c == 3:
            return from_left(e, 2)
        left = from_left(e, c - 1)
        return jnp.where(below(c), from_right(e, c), left)

    def send_parts(e, k, c, head):
        mask = below(c)
        if c < 3:
            out_r[k, q(c), :] = jnp.where(mask, head, 0.0) if c > 0 else head
        if c > 0:
            out_l[k, q(c - 1), :] = jnp.where(mask, 0.0, head) if c < 3 else head
        send(
            e,
            c, out_r.at[k, pl.ds(c * low, low)] if c < 3 else None,
            c - 1, out_l.at[k, pl.ds((c - 1) * low, low)] if c > 0 else None,
        )

    def add_parts(e, c, mine):
        if c < 3:
            mine = mine + from_left(e, c)
        if c > 0:
            mine = mine + from_right(e, c - 1)
        return mine

    def put(rows, value):
        hi, lo = halves(value)
        vec[rows, :nc] = hi
        vec[rows, nc:] = lo

    def mul(pieces, first=False, last=False):
        def rows(i, carry):
            at = pl.ds(pl.multiple_of(i * BLOCK, BLOCK), BLOCK)
            acc = None if first else twice[at, :]
            for k0, k1 in pieces:
                both = jnp.dot(s_hi[at, k0:k1], vec[k0:k1, :], preferred_element_type=F32)
                rest = jnp.dot(s_lo[at, k0:k1], vec[k0:k1, :nc], preferred_element_type=F32)
                part = both[:, :nc] + (both[:, nc:] + rest)
                acc = part if acc is None else acc + part
            twice[at, :] = acc
            if last:
                twice[pl.ds(pl.multiple_of(width + i * BLOCK, BLOCK), BLOCK), :] = acc
            return carry

        lax.fori_loop(0, width // BLOCK, rows, 0)

    def mul_quarters(cs, last=False):
        mul([(c * low, (c + 1) * low) for c in cs], last=last)

    def folded(first, count):
        return twice[pl.ds(width - off + first, count), :]

    def x_send(src, dst, sends, recvs):
        for k in range(1, nx):
            peer = lax.rem(ix + k, nx)
            pltpu.make_async_remote_copy(
                src_ref=src(peer), dst_ref=dst, send_sem=sends, recv_sem=recvs,
                device_id=(peer, iy), device_id_type=MESH,
            ).start()

    def y_send(src, dst, sends, recvs):
        def go(k, carry):
            peer = lax.rem(iy + k, ny)
            pltpu.make_async_remote_copy(
                src_ref=src(peer), dst_ref=dst, send_sem=sends, recv_sem=recvs,
                device_id=(ix, peer), device_id_type=MESH,
            ).start()
            return carry

        lax.fori_loop(1, ny, go, 0)

    def wait_for(ref, count, sem):
        view = ref.at[pl.ds(0, count)]
        pltpu.make_async_copy(view, view, sem).wait()

    def red(r):
        return [s[name + str(r)] for name in ("pa", "fa", "pb", "fb", "ga", "gb")]

    def red1(r, value):
        pa, fa = red(r)[:2]
        h = value.shape[0] // nx
        for i in range(nx):
            pa[i] = value[i * h : (i + 1) * h]
        x_send(lambda peer: pa.at[peer], fa.at[ix], s["rs"].at[r, 0], s["rr"].at[r, 0])
        fa[ix] = pa[ix]

    def red2(r):
        _, fa, pb, fb = red(r)[:4]
        wait_for(fa, nx - 1, s["rr"].at[r, 0])
        total = jnp.sum(fa[...], axis=0)
        h = total.shape[0] // ny
        for i in range(ny):
            pb[i] = total[i * h : (i + 1) * h]
        y_send(lambda peer: pb.at[peer], fb.at[iy], s["rs"].at[r, 1], s["rr"].at[r, 1])
        fb[iy] = pb[iy]

    def red3(r):
        fb, ga = red(r)[3:5]
        wait_for(fb, ny - 1, s["rr"].at[r, 1])
        ga[iy] = jnp.sum(fb[...], axis=0)
        y_send(lambda peer: ga.at[iy], ga.at[iy], s["rs"].at[r, 2], s["rr"].at[r, 2])

    def red4(r):
        ga, gb = red(r)[4:]
        wait_for(ga, ny - 1, s["rr"].at[r, 2])
        x_send(lambda peer: ga, gb.at[ix], s["rs"].at[r, 3], s["rr"].at[r, 3])
        gb[ix] = ga[...]

    def red5(r):
        gb = red(r)[5]
        wait_for(gb, nx - 1, s["rr"].at[r, 3])
        h = gb.shape[2]
        for i in range(nx):
            for j in range(ny):
                m_ref[(i * ny + j) * h : (i * ny + j + 1) * h, :] = gb[i, j]
        return m_ref[: n * h, :]

    def scal1(it):
        x_send(lambda peer: scal_in.at[it], scal_x.at[it, ix], s["ss"].at[it, 0], s["sr"].at[it, 0])
        scal_x[it, ix] = scal_in[it]

    def scal2(it):
        wait_for(scal_x.at[it], nx - 1, s["sr"].at[it, 0])
        scal_mid[it] = jnp.sum(scal_x[it], axis=0)
        y_send(lambda peer: scal_mid.at[it], scal_y.at[it, iy], s["ss"].at[it, 1], s["sr"].at[it, 1])
        scal_y[it, iy] = scal_mid[it]

    def scal3(it):
        wait_for(scal_y.at[it], ny - 1, s["sr"].at[it, 1])
        sums = jnp.sum(scal_y[it], axis=0)
        return sums[0:1], sums[1:2], sums[2:3]

    turn, twist = lax.div(off, LANES), lax.rem(off, LANES)
    wraps = lax.broadcasted_iota(jnp.int32, (CHUNK, LANES), 1) < twist

    def split(g, carry):
        for slot in range(SLOTS):
            i = g * SLOTS + slot
            fetch(i, slot).wait()
            at = pl.ds(pl.multiple_of(i * CHUNK, CHUNK), CHUNK)

            def rolled(j):
                m = lax.rem(j - turn + tiles, tiles) * LANES
                return pltpu.roll(stages[slot][:, pl.ds(m, LANES)], twist, 1)

            before = rolled(-1)
            for j in range(tiles):
                now = rolled(j)
                hi, lo = halves(jnp.where(wraps, before, now))
                s_hi[at, j * LANES : (j + 1) * LANES] = hi
                s_lo[at, j * LANES : (j + 1) * LANES] = lo
                before = now

            @pl.when(i + SLOTS < chunks)
            def _():
                fetch(i + SLOTS, slot).start()

        return carry

    groups = chunks // SLOTS

    load_in(0).wait()
    corners = jnp.where(turns_left, 1, 0) + jnp.where(turns_right, 1, 0)
    pl.semaphore_wait(barrier, nx + ny - 2 + corners)

    send_own(0, 1, basis_own)
    load_in(1).wait()
    own_t = basis_own[...].T
    both = dot(own_t, jnp.concatenate([basis_own[...], right[...]], axis=1))
    red1(0, both[:, :nc])
    m_ref[nc:, :] = both[:, nc:]
    lax.fori_loop(0, groups // 4, split, 0)
    send_own(0, 2, basis_own)
    lax.fori_loop(groups // 4, groups // 2, split, 0)
    red2(0)
    for c in STEPS[2]:
        send_own(0, c, basis_own)
    lax.fori_loop(groups // 2, groups, split, 0)
    basis_w[slab:, :] = basis_own[...]
    put(slice(slab, width), basis_own[...])
    mul([(slab, width)], first=True)
    red3(0)
    for step, cs in enumerate(STEPS):
        for c in cs:
            value = halo(0, c)
            basis_w[q(c), :] = value
            put(q(c), value)
        mul_quarters(cs, last=step == 2)
    basis_hl[...] = vec[...]

    for cs in STEPS[:2]:
        for c in cs:
            head = folded(c * low, low)
            send_parts(1, 0, c, head)
            sc[q(c), :] = head
    for c in STEPS[2]:
        head = folded(c * low, low)
        send_parts(1, 0, c, head)
        sc[q(c), :] = head
    sc[slab:, :] = folded(slab, slab)
    red4(0)
    red1(1, jnp.concatenate([dot(basis_w[...].T, sc[...]), m_ref[nc:, :]], axis=0))
    sweep[...] = red5(0)
    sc_hl[:, :nc] = sc[...].astype(BF16)
    sc_hl[:, nc:] = (sc[...] - sc[...].astype(BF16).astype(F32)).astype(BF16)
    red2(1)

    lanes = lax.broadcasted_iota(jnp.int32, (nc, nc), 1)
    subs = lax.broadcasted_iota(jnp.int32, (nc, nc), 0)

    def eliminate(a, k, row, col, p):
        here = lanes == k
        inverse = 1.0 / p
        scaled = row * inverse
        new = a - col * scaled
        new = jnp.where(here, col * inverse, new)
        return jnp.where(subs == k, jnp.where(here, -inverse, scaled), new), scaled, inverse

    def pick(row, k):
        return jnp.sum(jnp.where(lanes[:1] == k, row, 0.0), axis=1, keepdims=True)

    def pivot(half, a):
        k = 2 * half
        row1, row2 = sweep[pl.ds(k, 1), :], sweep[pl.ds(k + 1, 1), :]
        col1 = jnp.sum(jnp.where(lanes == k, a, 0.0), axis=1, keepdims=True)
        col2 = jnp.sum(jnp.where(lanes == k + 1, a, 0.0), axis=1, keepdims=True)
        p1, cross, p2 = pick(row1, k), pick(row1, k + 1), pick(row2, k + 1)
        a, scaled, inverse = eliminate(a, k, row1, col1, p1)
        ratio = cross * inverse
        row2 = jnp.where(lanes[:1] == k, ratio, row2 - cross * scaled)
        col2 = jnp.where(subs[:, :1] == k, ratio, col2 - col1 * ratio)
        a, _, _ = eliminate(a, k + 1, row2, col2, p2 - cross * ratio)
        sweep[...] = a
        return a

    ginv = -lax.fori_loop(0, nc // 2, pivot, sweep[...])
    red3(1)
    load_in(2).wait()
    y0 = dot(ginv, load[...])
    y0_op = right_operand(y0)

    fc = s["fc"]
    for cs in STEPS:
        for c in cs:
            fc_c = add_parts(1, c, sc[own_q(c), :])
            fc[q(c), :] = fc_c
            img[0, own_q(c), :] = right[q(c), :] - small(narrow(fc_c), y0_op)
            send_own(2, c, img.at[0, pl.ds(slab, slab)])
    put(slice(slab, width), img[0, slab:, :])
    mul([(slab, width)], first=True)
    red4(1)
    lam[...] = small(basis_hl[slab:, :], y0_op)
    fc_hi, fc_lo = halves(fc[...].T)
    s["fct_hi"][...] = fc_hi
    s["fct_lo"][...] = fc_lo

    def coarse(rows):
        both = jnp.dot(s["fct_hi"][...], rows, preferred_element_type=F32)
        rest = jnp.dot(s["fct_lo"][...], rows[:, :nc], preferred_element_type=F32)
        return both[:, :nc] + (both[:, nc:] + rest)

    sums = red5(1)
    amp = dot(ginv, sums[nc:] - dot(sums[:nc], y0))

    def bases(op, step, beta, old):
        def rows(i, carry):
            at = pl.ds(pl.multiple_of(i * BLOCK, BLOCK), BLOCK)
            cs = small(basis_hl[at, :], op)
            ss = small(sc_hl[at, :], op)
            if step is None:
                zbase[at, :] = -cs
                base[at, :] = -ss
            elif beta is None:
                zbase[at, :] = z[at, :] + step * cs
                base[at, :] = p_ref[at, :] + step * ss
            else:
                zbase[at, :] = z[at, :] + step * (cs - beta * img[old, at, :])
                base[at, :] = p_ref[at, :] + step * (ss - beta * si[at, :])
            return carry

        lax.fori_loop(0, width // BLOCK, rows, 0)

    bases(right_operand(amp), None, None, None)
    z[slab:, :] = zbase[slab:, :] + img[0, slab:, :]
    red1(2, coarse(narrow(z[slab:, :])))

    energy = curvature = coarse_image = step = beta = None
    for it in range(ITERS):
        last = it == ITERS - 1
        e = 2 + 2 * it
        scale = 1.0 if it == 0 else -step
        r = 2 + it

        for k, cs in enumerate(STEPS):
            for c in cs:
                value = halo(e, c)
                img[it, q(c), :] = value
                put(q(c), value)
            mul_quarters(cs, last=k == 2)
            if k == 0:
                red2(r)

        for cs in STEPS[:2]:
            for c in cs:
                p_c = base[q(c), :] + scale * folded(c * low, low)
                p_ref[q(c), :] = p_c
                if not last:
                    send_parts(e + 1, 1 + it, c, p_c)
        for c in STEPS[2]:
            p_ref[q(c), :] = base[q(c), :] + scale * folded(c * low, low)
        if it == 1:
            pass
        p_ref[slab:, :] = base[slab:, :] + scale * folded(slab, slab)
        z[:slab, :] = zbase[:slab, :] + scale * img[it, :slab, :]
        scal_in[it, 0:1] = jnp.sum(z[...] * p_ref[...], axis=0, keepdims=True)
        scal_in[it, 1:2] = jnp.sum(z[slab:, :] * z[slab:, :], axis=0, keepdims=True)
        if it == 0:
            scal_in[it, 2:3] = jnp.zeros((1, nc), F32)
        else:
            own = img[it, slab:, :]
            if it > 1:
                own = own + beta * s["image"][...]
            s["image"][...] = own
            scal_in[it, 2:3] = jnp.sum(z[slab:, :] * own, axis=0, keepdims=True)
        scal_in[it, 3:4] = jnp.zeros((1, nc), F32)
        scal1(it)
        if it > 0 and not last:
            raw = folded(0, width)
            si[...] = raw if it == 1 else raw + beta * si[...]
        red3(r)
        scal2(it)
        if not last:
            for c in STEPS[2]:
                send_parts(e + 1, 1 + it, c, p_ref[q(c), :])
            for cs in STEPS[:2]:
                for c in cs:
                    img[it + 1, own_q(c), :] = add_parts(e + 1, c, p_ref[own_q(c), :])
                    send_own(e + 2, c, img.at[it + 1, pl.ds(slab, slab)])
        red4(r)
        curved, energy_now, crossed = scal3(it)
        if not last:
            for c in STEPS[2]:
                img[it + 1, own_q(c), :] = add_parts(e + 1, c, p_ref[own_q(c), :])
                send_own(e + 2, c, img.at[it + 1, pl.ds(slab, slab)])
            put(slice(slab, width), img[it + 1, slab:, :])
            mul([(slab, width)], first=True)
        coarse_now = red5(r)
        if it == 0:
            d[...] = z[slab:, :]
            curvature = curved
            coarse_image = coarse_now
        else:
            beta = energy_now / energy
            d[...] = z[slab:, :] + beta * d[...]
            curvature = curved + beta * (2.0 * crossed + beta * curvature)
            coarse_image = coarse_now + beta * coarse_image
        energy = energy_now
        step = energy / curvature
        lam[...] += step * d[...]
        shift = dot(ginv, coarse_image)
        amp = amp - step * shift
        if not last:
            bases(right_operand(shift), step, beta, it)
            z[slab:, :] = zbase[slab:, :] - step * img[it + 1, slab:, :]
            red1(r + 1, coarse(narrow(z[slab:, :])))

    amp_out[...] = amp
    out_lam = pltpu.make_async_copy(lam, lam_hbm, s["load_sem"].at[0])
    out_amp = pltpu.make_async_copy(amp_out, amp_hbm, s["load_sem"].at[1])
    out_lam.start()
    out_amp.start()

    for e in range(EXCHANGES):
        for i in range(3):
            @pl.when(me > 0)
            def _():
                to_left(e, i, any_part).wait_send()

            @pl.when(me < n - 1)
            def _():
                to_right(e, i, any_part).wait_send()

    for r in range(REDUCES):
        pa, _, pb, _, ga, gb = red(r)
        wait_for(pa, nx - 1, s["rs"].at[r, 0])
        wait_for(pb, ny - 1, s["rs"].at[r, 1])
        wait_for(ga, ny - 1, s["rs"].at[r, 2])
        wait_for(gb, nx - 1, s["rs"].at[r, 3])
    for it in range(ITERS):
        wait_for(scal_x.at[it], nx - 1, s["ss"].at[it, 0])
        wait_for(scal_y.at[it], ny - 1, s["ss"].at[it, 1])
    out_lam.wait()
    out_amp.wait()


def entry(nx, ny, names, *refs):
    fixed = len(refs) - len(names)
    kernel(nx, ny, *refs[:fixed], dict(zip(names, refs[fixed:])))


def solution(mesh):
    nx, ny = mesh.shape["gx"], mesh.shape["gy"]

    def local(schur_blocks, offsets, right_side, coarse_basis, coarse_load):
        slab, r = right_side.shape
        nc = coarse_basis.shape[1]
        width = schur_blocks.shape[1]
        span = slab - slab // 4
        vmem, dma = pltpu.VMEM, pltpu.SemaphoreType.DMA
        scratch = {"stage%d" % i: vmem((CHUNK, width), F32) for i in range(SLOTS)}
        scratch |= {name: vmem((width, width), BF16) for name in ("s_hi", "s_lo")}
        scratch |= {name: vmem((width, 2 * nc), BF16) for name in ("vec", "basis_hl", "sc_hl")}
        scratch |= {name: vmem((width, r), F32) for name in ("basis_w", "sc", "p", "z", "base", "zbase", "si")}
        scratch |= {name: vmem((slab, r), F32) for name in ("right", "basis_own", "lam", "d", "fc", "image")}
        scratch |= {name: vmem((nc, r), F32) for name in ("load", "amp", "sweep")}
        scratch |= {name: vmem((nc, slab), BF16) for name in ("fct_hi", "fct_lo")}
        scratch |= {
            "twice": vmem((2 * width, r), F32),
            "img": vmem((IMAGES, width, r), F32),
            "out_l": vmem((PARTS, span, r), F32),
            "out_r": vmem((PARTS, span, r), F32),
            "in_l": vmem((EXCHANGES, span, r), F32),
            "in_r": vmem((EXCHANGES, span, r), F32),
            "m": vmem((2 * nc, r), F32),
            "scal_in": vmem((ITERS, 4, r), F32),
            "scal_mid": vmem((ITERS, 4, r), F32),
            "scal_x": vmem((ITERS, nx, 4, r), F32),
            "scal_y": vmem((ITERS, ny, 4, r), F32),
        }
        for k in range(REDUCES):
            rows = 2 * nc if k == 1 else nc
            h, p = rows // nx, rows // (nx * ny)
            scratch |= {
                "pa%d" % k: vmem((nx, h, r), F32),
                "fa%d" % k: vmem((nx, h, r), F32),
                "pb%d" % k: vmem((ny, p, r), F32),
                "fb%d" % k: vmem((ny, p, r), F32),
                "ga%d" % k: vmem((ny, p, r), F32),
                "gb%d" % k: vmem((nx, ny, p, r), F32),
            }
        scratch |= {name: dma((EXCHANGES, 3)) for name in ("hs_l", "hs_r", "hr_l", "hr_r")}
        scratch |= {
            "stage_sem": dma((SLOTS,)),
            "load_sem": dma((3,)),
            "rs": dma((REDUCES, 4)),
            "rr": dma((REDUCES, 4)),
            "ss": dma((ITERS, 2)),
            "sr": dma((ITERS, 2)),
        }
        names = tuple(scratch)
        hbm = pl.BlockSpec(memory_space=pl.ANY)
        return pl.pallas_call(
            functools.partial(entry, nx, ny, names),
            out_shape=(
                jax.ShapeDtypeStruct((slab, r), F32),
                jax.ShapeDtypeStruct((nc, r), F32),
            ),
            in_specs=[pl.BlockSpec(memory_space=pltpu.SMEM), hbm, hbm, hbm, hbm],
            out_specs=(hbm, hbm),
            scratch_shapes=list(scratch.values()),
            compiler_params=pltpu.CompilerParams(
                collective_id=0, has_side_effects=True, vmem_limit_bytes=60 * 1024 * 1024
            ),
            name="projected_cg",
        )(offsets, schur_blocks[0], right_side, coarse_basis, coarse_load)

    in_specs = (
        P(("gx", "gy"), None, None),
        P(("gx", "gy")),
        P(("gx", "gy"), None),
        P(("gx", "gy"), None),
        P(),
    )
    out_specs = (P(("gx", "gy"), None), P())
    return jax.shard_map(local, mesh=mesh, in_specs=in_specs, out_specs=out_specs, check_vma=False)
```

```python
import functools

import jax
import jax.numpy as jnp
from jax import lax
from jax.experimental import pallas as pl
from jax.experimental.pallas import tpu as pltpu
from jax.sharding import PartitionSpec as P

ITERS = 3
MESH = pl.DeviceIdType.MESH
HIGHEST = lax.Precision.HIGHEST
F32 = jnp.float32
BF16 = jnp.bfloat16
LANES = 128
CHUNK = 128
SLOTS = 2
GROUP = 512
BLOCK = 512
PIVOTS = 4
EXCHANGES = 3 + 2 * (ITERS - 1)
PARTS = ITERS
IMAGES = ITERS
REDUCES = 1 + ITERS
STEPS = ((1,), (2,), (0, 3))


def dot(a, b):
    return jnp.dot(a, b, precision=HIGHEST, preferred_element_type=F32)


def halves(x):
    hi = x.astype(BF16)
    return hi, (x - hi.astype(F32)).astype(BF16)


def narrow(x):
    return jnp.concatenate(halves(x), axis=1)


def right_operand(x):
    hi, lo = halves(x)
    return jnp.concatenate(
        [jnp.concatenate([hi, lo], axis=1), jnp.concatenate([hi, jnp.zeros_like(lo)], axis=1)], axis=0
    )


def small(left, right):
    both = jnp.dot(left, right, preferred_element_type=F32)
    half = both.shape[1] // 2
    return both[:, :half] + both[:, half:]


def kernel(nx, ny, off_ref, schur_ref, right_hbm, basis_hbm, load_hbm, lam_hbm, amp_hbm, s):
    n = nx * ny
    slab, nc = s["right"].shape
    width = 2 * slab
    low = slab // 4
    span = slab - low
    ix, iy = lax.axis_index("gx"), lax.axis_index("gy")
    me = ix * ny + iy
    off = off_ref[0]
    groups = width // GROUP
    tiles = width // LANES
    stages = [s["stage%d" % i] for i in range(SLOTS)]
    s_hi, s_lo, vec, twice = s["s_hi"], s["s_lo"], s["vec"], s["twice"]
    in_l, in_r, out_l, out_r, img = s["in_l"], s["in_r"], s["out_l"], s["out_r"], s["img"]
    right, basis_own, load = s["right"], s["basis_own"], s["load"]
    basis_hl, sc, sc_hl = s["basis_hl"], s["sc"], s["sc_hl"]
    p_ref, z, base, zbase, si = s["p"], s["z"], s["base"], s["zbase"], s["si"]
    lam, amp_out, d = s["lam"], s["amp"], s["d"]
    m_ref, sweep = s["m"], s["sweep"]
    scal_in, scal_mid, scal_x, scal_y = s["scal_in"], s["scal_mid"], s["scal_x"], s["scal_y"]

    def where_is(i):
        return (lax.div(i, ny), lax.rem(i, ny))

    def fetch(i, slot):
        return pltpu.make_async_copy(
            schur_ref.at[pl.ds(i * GROUP, GROUP), :], stages[slot], s["stage_sem"].at[slot]
        )

    def load_in(k):
        src, dst = ((basis_hbm, basis_own), (right_hbm, right), (load_hbm, load))[k]
        return pltpu.make_async_copy(src, dst, s["load_sem"].at[k])

    load_in(0).start()
    barrier = pltpu.get_barrier_semaphore()

    def greet(x, y):
        pl.semaphore_signal(barrier, inc=1, device_id=(x, y), device_id_type=MESH)

    def greet_x(k, carry):
        greet(lax.rem(ix + k, nx), iy)
        return carry

    def greet_y(k, carry):
        greet(ix, lax.rem(iy + k, ny))
        return carry

    turns_left = jnp.logical_and(iy == 0, ix > 0)
    turns_right = jnp.logical_and(iy == ny - 1, ix < nx - 1)

    lax.fori_loop(1, nx, greet_x, 0)
    lax.fori_loop(1, ny, greet_y, 0)

    @pl.when(turns_left)
    def _():
        greet(ix - 1, ny - 1)

    @pl.when(turns_right)
    def _():
        greet(ix + 1, 0)

    load_in(1).start()
    for i in range(SLOTS):
        fetch(i, i).start()
    load_in(2).start()

    @pl.when(me == 0)
    def _():
        in_l[...] = jnp.zeros_like(in_l)

    @pl.when(me == n - 1)
    def _():
        in_r[...] = jnp.zeros_like(in_r)

    def to_right(e, i, src):
        return pltpu.make_async_remote_copy(
            src_ref=src, dst_ref=in_l.at[e, pl.ds(i * low, low)], send_sem=s["hs_r"].at[e, i],
            recv_sem=s["hr_l"].at[e, i], device_id=where_is(lax.rem(me + 1, n)), device_id_type=MESH,
        )

    def to_left(e, i, src):
        return pltpu.make_async_remote_copy(
            src_ref=src, dst_ref=in_r.at[e, pl.ds(i * low, low)], send_sem=s["hs_l"].at[e, i],
            recv_sem=s["hr_r"].at[e, i], device_id=where_is(lax.rem(me + n - 1, n)), device_id_type=MESH,
        )

    any_part = out_l.at[0, pl.ds(0, low)]

    def send(e, i_right, src_right, i_left, src_left):
        if src_left is not None:
            @pl.when(me > 0)
            def _():
                to_left(e, i_left, src_left).start()

        if src_right is not None:
            @pl.when(me < n - 1)
            def _():
                to_right(e, i_right, src_right).start()

    def from_left(e, i):
        @pl.when(me > 0)
        def _():
            to_right(e, i, any_part).wait_recv()

        return in_l[e, i * low : (i + 1) * low, :]

    def from_right(e, i):
        @pl.when(me < n - 1)
        def _():
            to_left(e, i, any_part).wait_recv()

        return in_r[e, i * low : (i + 1) * low, :]

    def below(c):
        return lax.broadcasted_iota(jnp.int32, (low, nc), 0) + c * low < off

    def q(c):
        return slice(c * low, (c + 1) * low)

    def own_q(c):
        return slice(slab + c * low, slab + (c + 1) * low)

    def send_own(e, c, ref):
        view = ref.at[pl.ds(c * low, low)]
        send(e, c - 1, view if c > 0 else None, c, view if c < 3 else None)

    def halo(e, c):
        if c == 0:
            return from_right(e, 0)
        if c == 3:
            return from_left(e, 2)
        left = from_left(e, c - 1)
        return jnp.where(below(c), from_right(e, c), left)

    def send_parts(e, k, c, head):
        mask = below(c)
        if c < 3:
            out_r[k, q(c), :] = jnp.where(mask, head, 0.0) if c > 0 else head
        if c > 0:
            out_l[k, q(c - 1), :] = jnp.where(mask, 0.0, head) if c < 3 else head
        send(
            e,
            c, out_r.at[k, pl.ds(c * low, low)] if c < 3 else None,
            c - 1, out_l.at[k, pl.ds((c - 1) * low, low)] if c > 0 else None,
        )

    def add_parts(e, c, mine):
        if c < 3:
            mine = mine + from_left(e, c)
        if c > 0:
            mine = mine + from_right(e, c - 1)
        return mine

    def put(rows, value):
        hi, lo = halves(value)
        vec[rows, :nc] = hi
        vec[rows, nc:] = lo

    def product(at, pieces):
        total = None
        for k0, k1 in pieces:
            both = jnp.dot(s_hi[at, k0:k1], vec[k0:k1, :], preferred_element_type=F32)
            rest = jnp.dot(s_lo[at, k0:k1], vec[k0:k1, :nc], preferred_element_type=F32)
            part = both[:, :nc] + (both[:, nc:] + rest)
            total = part if total is None else total + part
        return total

    def mul(pieces, first=False, last=False):
        tall = width if not first else slab

        def rows(i, carry):
            at = pl.ds(pl.multiple_of(i * tall, tall), tall)
            acc = product(at, pieces)
            if not first:
                acc = twice[at, :] + acc
            twice[at, :] = acc
            if last:
                twice[pl.ds(pl.multiple_of(width + i * tall, tall), tall), :] = acc
            return carry

        lax.fori_loop(0, width // tall, rows, 0)

    def mul_quarters(cs, last=False):
        mul([(c * low, (c + 1) * low) for c in cs], last=last)

    def folded(first, count):
        return twice[pl.ds(width - off + first, count), :]

    def x_send(src, dst, sends, recvs):
        for k in range(1, nx):
            peer = lax.rem(ix + k, nx)
            pltpu.make_async_remote_copy(
                src_ref=src(peer), dst_ref=dst, send_sem=sends, recv_sem=recvs,
                device_id=(peer, iy), device_id_type=MESH,
            ).start()

    def y_send(src, dst, sends, recvs):
        def go(k, carry):
            peer = lax.rem(iy + k, ny)
            pltpu.make_async_remote_copy(
                src_ref=src(peer), dst_ref=dst, send_sem=sends, recv_sem=recvs,
                device_id=(ix, peer), device_id_type=MESH,
            ).start()
            return carry

        lax.fori_loop(1, ny, go, 0)

    def wait_for(ref, count, sem):
        view = ref.at[pl.ds(0, count)]
        pltpu.make_async_copy(view, view, sem).wait()

    def red(r):
        return [s[name + str(r)] for name in ("pa", "fa", "pb", "fb", "ga", "gb")]

    def red1(r, value):
        pa, fa = red(r)[:2]
        h = value.shape[0] // nx
        for i in range(nx):
            pa[i] = value[i * h : (i + 1) * h]
        x_send(lambda peer: pa.at[peer], fa.at[ix], s["rs"].at[r, 0], s["rr"].at[r, 0])
        fa[ix] = pa[ix]

    def red2(r):
        _, fa, pb, fb = red(r)[:4]
        wait_for(fa, nx - 1, s["rr"].at[r, 0])
        total = jnp.sum(fa[...], axis=0)
        h = total.shape[0] // ny
        for i in range(ny):
            pb[i] = total[i * h : (i + 1) * h]
        y_send(lambda peer: pb.at[peer], fb.at[iy], s["rs"].at[r, 1], s["rr"].at[r, 1])
        fb[iy] = pb[iy]

    def red3(r):
        fb, ga = red(r)[3:5]
        wait_for(fb, ny - 1, s["rr"].at[r, 1])
        ga[iy] = jnp.sum(fb[...], axis=0)
        y_send(lambda peer: ga.at[iy], ga.at[iy], s["rs"].at[r, 2], s["rr"].at[r, 2])

    def red4(r):
        ga, gb = red(r)[4:]
        wait_for(ga, ny - 1, s["rr"].at[r, 2])
        x_send(lambda peer: ga, gb.at[ix], s["rs"].at[r, 3], s["rr"].at[r, 3])
        gb[ix] = ga[...]

    def red5(r):
        gb = red(r)[5]
        wait_for(gb, nx - 1, s["rr"].at[r, 3])
        h = gb.shape[2]
        for i in range(nx):
            for j in range(ny):
                m_ref[(i * ny + j) * h : (i * ny + j + 1) * h, :] = gb[i, j]
        return m_ref[: n * h, :]

    def scal1(it):
        y_send(lambda peer: scal_in.at[it], scal_y.at[it, iy], s["ss"].at[it, 1], s["sr"].at[it, 1])
        scal_y[it, iy] = scal_in[it]

    def scal2(it):
        wait_for(scal_y.at[it], ny - 1, s["sr"].at[it, 1])
        scal_mid[it] = jnp.sum(scal_y[it], axis=0)
        x_send(lambda peer: scal_mid.at[it], scal_x.at[it, ix], s["ss"].at[it, 0], s["sr"].at[it, 0])
        scal_x[it, ix] = scal_mid[it]

    def scal3(it):
        wait_for(scal_x.at[it], nx - 1, s["sr"].at[it, 0])
        sums = jnp.sum(scal_x[it], axis=0)
        return sums[0:1], sums[1:2], sums[2:3]

    def scal_all(it):
        all_send(lambda peer: scal_in.at[it], s["scal_a"].at[me], s["ss"].at[it, 0], s["sr"].at[it, 0])
        s["scal_a"][me] = scal_in[it]

    def scal_sum(it):
        wait_for(s["scal_a"], n - 1, s["sr"].at[it, 0])
        sums = jnp.sum(s["scal_a"][...], axis=0)
        return sums[0:1], sums[1:2], sums[2:3]

    def all_send(src, dst, sends, recvs):
        def go(k, carry):
            peer = lax.rem(me + k, n)
            pltpu.make_async_remote_copy(
                src_ref=src(peer), dst_ref=dst, send_sem=sends, recv_sem=recvs,
                device_id=where_is(peer), device_id_type=MESH,
            ).start()
            return carry

        lax.fori_loop(1, n, go, 0)

    def direct1(value):
        h = value.shape[0] // n
        for i in range(n):
            s["dp"][i] = value[i * h : (i + 1) * h]
        all_send(lambda peer: s["dp"].at[peer], s["df"].at[me], s["ds"].at[0], s["dr"].at[0])
        s["df"][me] = s["dp"][me]

    def direct2():
        wait_for(s["df"], n - 1, s["dr"].at[0])
        s["dt"][me] = jnp.sum(s["df"][...], axis=0)
        all_send(lambda peer: s["dt"].at[me], s["dt"].at[me], s["ds"].at[1], s["dr"].at[1])

    def direct3():
        wait_for(s["dt"], n - 1, s["dr"].at[1])
        h = s["dt"].shape[1]
        for i in range(n):
            m_ref[i * h : (i + 1) * h, :] = s["dt"][i]
        return m_ref[: n * h, :]

    turn, twist = lax.div(off, LANES), lax.rem(off, LANES)
    wraps = lax.broadcasted_iota(jnp.int32, (CHUNK, LANES), 1) < twist

    def split(g):
        slot = g % SLOTS
        fetch(g, slot).wait()
        for i in range(GROUP // CHUNK):
            rows = slice(i * CHUNK, (i + 1) * CHUNK)
            at = slice(g * GROUP + i * CHUNK, g * GROUP + (i + 1) * CHUNK)

            def rolled(j):
                m = lax.rem(j - turn + tiles, tiles) * LANES
                return pltpu.roll(stages[slot][rows, pl.ds(m, LANES)], twist, 1)

            before = rolled(-1)
            for j in range(tiles):
                now = rolled(j)
                hi, lo = halves(jnp.where(wraps, before, now))
                s_hi[at, j * LANES : (j + 1) * LANES] = hi
                s_lo[at, j * LANES : (j + 1) * LANES] = lo
                before = now
        if g + SLOTS < groups:
            fetch(g + SLOTS, slot).start()

    def mul_group(g):
        at = slice(g * GROUP, (g + 1) * GROUP)
        twice[at, :] = product(at, [(slab, width)])

    load_in(0).wait()
    load_in(1).wait()
    own_t = basis_own[...].T
    both = dot(own_t, jnp.concatenate([basis_own[...], right[...]], axis=1))
    m_ref[nc:, :] = both[:, nc:]
    hi, lo = halves(own_t)
    s["bt_hi"][:, slab:] = hi
    s["bt_lo"][:, slab:] = lo
    put(slice(slab, width), basis_own[...])
    corners = jnp.where(turns_left, 1, 0) + jnp.where(turns_right, 1, 0)
    pl.semaphore_wait(barrier, nx + ny - 2 + corners)

    red1(0, both[:, :nc])
    send_own(0, 1, basis_own)
    split(0)
    mul_group(0)
    split(1)
    red2(0)
    for c in STEPS[1]:
        send_own(0, c, basis_own)
    for g in range(2, groups):
        mul_group(g - 1)
        split(g)
    red3(0)
    for c in STEPS[2]:
        send_own(0, c, basis_own)
    mul_group(groups - 1)
    for step, cs in enumerate(STEPS):
        for c in cs:
            value = halo(0, c)
            hi, lo = halves(value.T)
            s["bt_hi"][:, q(c)] = hi
            s["bt_lo"][:, q(c)] = lo
            put(q(c), value)
        mul_quarters(cs, last=step == 2)
        if step == 1:
            red4(0)
    basis_hl[...] = vec[...]

    for cs in STEPS[:2]:
        for c in cs:
            head = folded(c * low, low)
            send_parts(1, 0, c, head)
            sc[q(c), :] = head
    for c in STEPS[2]:
        head = folded(c * low, low)
        send_parts(1, 0, c, head)
        sc[q(c), :] = head
    sc[slab:, :] = folded(slab, slab)
    sc_hl[...] = narrow(sc[...])
    both = jnp.dot(s["bt_hi"][...], sc_hl[...], preferred_element_type=F32)
    rest = jnp.dot(s["bt_lo"][...], sc_hl[:, :nc], preferred_element_type=F32)
    red1(1, jnp.concatenate([both[:, :nc] + (both[:, nc:] + rest), m_ref[nc:, :]], axis=0))
    sweep[...] = red5(0)

    lanes = lax.broadcasted_iota(jnp.int32, (nc, nc), 1)
    subs = lax.broadcasted_iota(jnp.int32, (nc, nc), 0)

    def eliminate(a, k, row, col, p):
        here = lanes == k
        inverse = 1.0 / p
        scaled = row * inverse
        new = a - col * scaled
        new = jnp.where(here, col * inverse, new)
        return jnp.where(subs == k, jnp.where(here, -inverse, scaled), new), scaled, inverse

    def pick(row, k):
        return jnp.sum(jnp.where(lanes[:1] == k, row, 0.0), axis=1, keepdims=True)

    def pivot(turn, a):
        k = PIVOTS * turn
        some = range(PIVOTS)
        rows = [sweep[pl.ds(k + i, 1), :] for i in some]
        cols = [jnp.sum(jnp.where(lanes == k + i, a, 0.0), axis=1, keepdims=True) for i in some]
        block = {(i, j): pick(rows[i], k + j) for i in some for j in some if i <= j}
        for i in some:
            a, scaled, inverse = eliminate(a, k + i, rows[i], cols[i], block[i, i])
            for j in range(i + 1, PIVOTS):
                ratio = block[i, j] * inverse
                rows[j] = jnp.where(lanes[:1] == k + i, ratio, rows[j] - block[i, j] * scaled)
                cols[j] = jnp.where(subs[:, :1] == k + i, ratio, cols[j] - cols[i] * ratio)
                for l in range(j, PIVOTS):
                    block[j, l] = block[j, l] - ratio * block[i, l]
        sweep[...] = a
        return a

    half_way = lax.fori_loop(0, nc // PIVOTS // 2, pivot, sweep[...])
    red2(1)
    ginv = -lax.fori_loop(nc // PIVOTS // 2, nc // PIVOTS, pivot, half_way)
    load_in(2).wait()
    y0 = dot(ginv, load[...])
    y0_op = right_operand(y0)

    fc = s["fc"]
    for cs in STEPS:
        for c in cs:
            fc_c = add_parts(1, c, sc[own_q(c), :])
            fc[q(c), :] = fc_c
            img[0, own_q(c), :] = right[q(c), :] - small(narrow(fc_c), y0_op)
            send_own(2, c, img.at[0, pl.ds(slab, slab)])
        if cs == STEPS[0]:
            red3(1)
    fc_hi, fc_lo = halves(fc[...].T)
    s["fct_hi"][...] = fc_hi
    s["fct_lo"][...] = fc_lo

    def coarse(rows):
        both = jnp.dot(s["fct_hi"][...], rows, preferred_element_type=F32)
        rest = jnp.dot(s["fct_lo"][...], rows[:, :nc], preferred_element_type=F32)
        return both[:, :nc] + (both[:, nc:] + rest)

    red1(2, coarse(narrow(img[0, slab:, :])))
    put(slice(slab, width), img[0, slab:, :])
    mul([(slab, width)], first=True)
    red4(1)
    red2(2)
    lam[...] = small(basis_hl[slab:, :], y0_op)

    def own_z(op, step, beta, old):
        cs = small(basis_hl[slab:, :], op)
        if step is None:
            z[slab:, :] = img[old, slab:, :] - cs
        elif beta is None:
            z[slab:, :] = z[slab:, :] + step * (cs - img[old + 1, slab:, :])
        else:
            z[slab:, :] = z[slab:, :] + step * (cs - beta * img[old, slab:, :] - img[old + 1, slab:, :])

    def bases(op, step, beta, old):
        def rows(i, carry):
            at = pl.ds(pl.multiple_of(i * BLOCK, BLOCK), BLOCK)
            ss = small(sc_hl[at, :], op)
            if step is None:
                base[at, :] = -ss
            elif beta is None:
                base[at, :] = p_ref[at, :] + step * ss
            else:
                base[at, :] = p_ref[at, :] + step * (ss - beta * si[at, :])
            return carry

        def halo_rows(i, carry):
            at = pl.ds(pl.multiple_of(i * BLOCK, BLOCK), BLOCK)
            cs = small(basis_hl[at, :], op)
            if step is None:
                zbase[at, :] = -cs
            elif beta is None:
                zbase[at, :] = z[at, :] + step * cs
            else:
                zbase[at, :] = z[at, :] + step * (cs - beta * img[old, at, :])
            return carry

        lax.fori_loop(0, width // BLOCK, rows, 0)
        lax.fori_loop(0, slab // BLOCK, halo_rows, 0)

    def own_scalars(it, beta):
        mine = z[slab:, :]
        scal_in[it, 1:2] = jnp.sum(mine * mine, axis=0, keepdims=True)
        scal_in[it, 3:4] = jnp.zeros((1, nc), F32)
        if it == 0:
            scal_in[it, 2:3] = jnp.zeros((1, nc), F32)
            return
        image = img[it, slab:, :]
        if it > 1:
            image = image + beta * s["image"][...]
        s["image"][...] = image
        scal_in[it, 2:3] = jnp.sum(mine * image, axis=0, keepdims=True)

    energy = curvature = coarse_image = step = beta = None
    for it in range(ITERS):
        last = it == ITERS - 1
        e = 2 + 2 * it
        scale = 1.0 if it == 0 else -step
        r = 2 + it

        for k, cs in enumerate(STEPS):
            for c in cs:
                value = halo(e, c)
                img[it, q(c), :] = value
                put(q(c), value)
            mul_quarters(cs, last=k == 2)
            if k == 0 and it == 0:
                sums = red5(1)
                cfc = s["cfc"]
                cfc[...] = sums[:nc]
                amp = dot(ginv, sums[nc:] - dot(cfc[...], y0))
                known = -dot(cfc[...], amp)
                op = right_operand(amp)
                own_z(op, None, None, 0)
                own_scalars(0, None)
                bases(op, None, None, 0)

        if last:
            direct2()

        def next_p(c):
            p_c = base[q(c), :] + scale * folded(c * low, low)
            p_ref[q(c), :] = p_c
            if not last:
                send_parts(e + 1, 1 + it, c, p_c)

        for c in STEPS[0]:
            next_p(c)
        for c in STEPS[1] + STEPS[2]:
            p_ref[q(c), :] = base[q(c), :] + scale * folded(c * low, low)
        p_ref[slab:, :] = base[slab:, :] + scale * folded(slab, slab)
        z[:slab, :] = zbase[:slab, :] + scale * img[it, :slab, :]
        scal_in[it, 0:1] = jnp.sum(z[...] * p_ref[...], axis=0, keepdims=True)
        if last:
            scal_all(it)
        else:
            scal1(it)
        if not last:
            red3(r)
            for c in STEPS[1] + STEPS[2]:
                send_parts(e + 1, 1 + it, c, p_ref[q(c), :])
        if it > 0 and not last:
            raw = folded(0, width)
            si[...] = raw if it == 1 else raw + beta * si[...]

        def next_image(cs):
            for c in cs:
                value = add_parts(e + 1, c, p_ref[own_q(c), :])
                img[it + 1, own_q(c), :] = value
                send_own(e + 2, c, img.at[it + 1, pl.ds(slab, slab)])
                put(own_q(c), value)

        def mul_own(cs):
            mul([(slab + c * low, slab + (c + 1) * low) for c in cs], first=cs == STEPS[0])

        if not last:
            next_image(STEPS[0])
            mul_own(STEPS[0])
        if not last:
            scal2(it)
            red4(r)
        if not last:
            next_image(STEPS[1])
            mul_own(STEPS[1])
        curved, energy_now, crossed = scal_sum(it) if last else scal3(it)
        raw_coarse = direct3() if last else red5(r)
        if it == 0:
            coarse_z = known + raw_coarse
            coarse_image = coarse_z
            d[...] = z[slab:, :]
            curvature = curved
        else:
            images = raw_coarse if it == 1 else raw_coarse + beta * images
            coarse_z = known - step * images
            beta = energy_now / energy
            d[...] = z[slab:, :] + beta * d[...]
            curvature = curved + beta * (2.0 * crossed + beta * curvature)
            coarse_image = coarse_z + beta * coarse_image
        energy = energy_now
        step = energy / curvature
        lam[...] += step * d[...]
        shift = dot(ginv, coarse_image)
        amp = amp - step * shift
        if not last:
            op = right_operand(shift)
            bases(op, step, beta, it)
            next_image(STEPS[2])
            local = coarse(narrow(img[it + 1, slab:, :]))
            if it + 1 < ITERS - 1:
                red1(r + 1, local)
            else:
                direct1(local)
            own_z(op, step, beta, it)
            own_scalars(it + 1, beta)
            mul_own(STEPS[2])
            known = coarse_z + step * dot(cfc[...], shift)
            if it + 1 < ITERS - 1:
                red2(r + 1)

    amp_out[...] = amp
    out_lam = pltpu.make_async_copy(lam, lam_hbm, s["load_sem"].at[0])
    out_amp = pltpu.make_async_copy(amp_out, amp_hbm, s["load_sem"].at[1])
    out_lam.start()
    out_amp.start()

    for e in range(EXCHANGES):
        for i in range(3):
            @pl.when(me > 0)
            def _():
                to_left(e, i, any_part).wait_send()

            @pl.when(me < n - 1)
            def _():
                to_right(e, i, any_part).wait_send()

    for r in range(REDUCES):
        pa, _, pb, _, ga, gb = red(r)
        wait_for(pa, nx - 1, s["rs"].at[r, 0])
        wait_for(pb, ny - 1, s["rs"].at[r, 1])
        wait_for(ga, ny - 1, s["rs"].at[r, 2])
        wait_for(gb, nx - 1, s["rs"].at[r, 3])
    wait_for(s["scal_a"], n - 1, s["ss"].at[ITERS - 1, 0])
    wait_for(s["dp"], n - 1, s["ds"].at[0])
    wait_for(s["dt"], n - 1, s["ds"].at[1])
    for it in range(ITERS - 1):
        wait_for(scal_x.at[it], nx - 1, s["ss"].at[it, 0])
        wait_for(scal_y.at[it], ny - 1, s["ss"].at[it, 1])
    out_lam.wait()
    out_amp.wait()


def entry(nx, ny, names, *refs):
    fixed = len(refs) - len(names)
    kernel(nx, ny, *refs[:fixed], dict(zip(names, refs[fixed:])))


def solution(mesh):
    nx, ny = mesh.shape["gx"], mesh.shape["gy"]

    def local(schur_blocks, offsets, right_side, coarse_basis, coarse_load):
        slab, r = right_side.shape
        nc = coarse_basis.shape[1]
        width = schur_blocks.shape[1]
        span = slab - slab // 4
        vmem, dma = pltpu.VMEM, pltpu.SemaphoreType.DMA
        scratch = {"stage%d" % i: vmem((GROUP, width), F32) for i in range(SLOTS)}
        scratch |= {name: vmem((width, width), BF16) for name in ("s_hi", "s_lo")}
        scratch |= {name: vmem((width, 2 * nc), BF16) for name in ("vec", "basis_hl", "sc_hl")}
        scratch |= {name: vmem((width, r), F32) for name in ("sc", "p", "z", "base", "zbase", "si")}
        scratch |= {name: vmem((slab, r), F32) for name in ("right", "basis_own", "lam", "d", "fc", "image")}
        scratch |= {name: vmem((nc, r), F32) for name in ("load", "amp", "sweep", "cfc")}
        scratch |= {name: vmem((nc, slab), BF16) for name in ("fct_hi", "fct_lo")}
        scratch |= {name: vmem((nc, width), BF16) for name in ("bt_hi", "bt_lo")}
        scratch |= {
            "twice": vmem((2 * width, r), F32),
            "img": vmem((IMAGES, width, r), F32),
            "out_l": vmem((PARTS, span, r), F32),
            "out_r": vmem((PARTS, span, r), F32),
            "in_l": vmem((EXCHANGES, span, r), F32),
            "in_r": vmem((EXCHANGES, span, r), F32),
            "m": vmem((2 * nc, r), F32),
            "scal_in": vmem((ITERS, 4, r), F32),
            "scal_mid": vmem((ITERS, 4, r), F32),
            "scal_a": vmem((nx * ny, 4, r), F32),
            "scal_x": vmem((ITERS, nx, 4, r), F32),
            "scal_y": vmem((ITERS, ny, 4, r), F32),
        }
        for k in range(REDUCES):
            rows = 2 * nc if k == 1 else nc
            h, p = rows // nx, rows // (nx * ny)
            scratch |= {
                "pa%d" % k: vmem((nx, h, r), F32),
                "fa%d" % k: vmem((nx, h, r), F32),
                "pb%d" % k: vmem((ny, p, r), F32),
                "fb%d" % k: vmem((ny, p, r), F32),
                "ga%d" % k: vmem((ny, p, r), F32),
                "gb%d" % k: vmem((nx, ny, p, r), F32),
            }
        scratch |= {name: vmem((nx * ny, nc // (nx * ny), r), F32) for name in ("dp", "df", "dt")}
        scratch |= {name: dma((EXCHANGES, 3)) for name in ("hs_l", "hs_r", "hr_l", "hr_r")}
        scratch |= {
            "ds": dma((2,)),
            "dr": dma((2,)),
            "stage_sem": dma((SLOTS,)),
            "load_sem": dma((3,)),
            "rs": dma((REDUCES, 4)),
            "rr": dma((REDUCES, 4)),
            "ss": dma((ITERS, 2)),
            "sr": dma((ITERS, 2)),
        }
        names = tuple(scratch)
        hbm = pl.BlockSpec(memory_space=pl.ANY)
        return pl.pallas_call(
            functools.partial(entry, nx, ny, names),
            out_shape=(
                jax.ShapeDtypeStruct((slab, r), F32),
                jax.ShapeDtypeStruct((nc, r), F32),
            ),
            in_specs=[pl.BlockSpec(memory_space=pltpu.SMEM), hbm, hbm, hbm, hbm],
            out_specs=(hbm, hbm),
            scratch_shapes=list(scratch.values()),
            compiler_params=pltpu.CompilerParams(
                collective_id=0, has_side_effects=True, vmem_limit_bytes=60 * 1024 * 1024
            ),
            name="projected_cg",
        )(offsets, schur_blocks[0], right_side, coarse_basis, coarse_load)

    in_specs = (
        P(("gx", "gy"), None, None),
        P(("gx", "gy")),
        P(("gx", "gy"), None),
        P(("gx", "gy"), None),
        P(),
    )
    out_specs = (P(("gx", "gy"), None), P())
    return jax.shard_map(local, mesh=mesh, in_specs=in_specs, out_specs=out_specs, check_vma=False)
```

```python
import functools

import jax
import jax.numpy as jnp
from jax import lax
from jax.experimental import pallas as pl
from jax.experimental.pallas import tpu as pltpu
from jax.sharding import PartitionSpec as P

ITERS = 3
MESH = pl.DeviceIdType.MESH
HIGHEST = lax.Precision.HIGHEST
F32 = jnp.float32
BF16 = jnp.bfloat16
LANES = 128
CHUNK = 128
SLOTS = 2
GROUP = 512
BLOCK = 1024
PIVOTS = 4
EXCHANGES = 3 + 2 * (ITERS - 1)
PARTS = ITERS
IMAGES = ITERS
REDUCES = 1 + ITERS
STEPS = ((1,), (2,), (0, 3))


def dot(a, b):
    return jnp.dot(a, b, precision=HIGHEST, preferred_element_type=F32)


def halves(x):
    hi = x.astype(BF16)
    return hi, (x - hi.astype(F32)).astype(BF16)


def narrow(x):
    return jnp.concatenate(halves(x), axis=1)


def right_operand(x):
    hi, lo = halves(x)
    return jnp.concatenate(
        [jnp.concatenate([hi, lo], axis=1), jnp.concatenate([hi, jnp.zeros_like(lo)], axis=1)], axis=0
    )


def small(left, right):
    both = jnp.dot(left, right, preferred_element_type=F32)
    half = both.shape[1] // 2
    return both[:, :half] + both[:, half:]


def kernel(nx, ny, off_ref, schur_ref, right_hbm, basis_hbm, load_hbm, lam_hbm, amp_hbm, s):
    n = nx * ny
    slab, nc = s["right"].shape
    width = 2 * slab
    low = slab // 4
    span = slab - low
    ix, iy = lax.axis_index("gx"), lax.axis_index("gy")
    me = ix * ny + iy
    off = off_ref[0]
    groups = width // GROUP
    tiles = width // LANES
    stages = [s["stage%d" % i] for i in range(SLOTS)]
    s_hi, s_lo, vec, twice = s["s_hi"], s["s_lo"], s["vec"], s["twice"]
    in_l, in_r, out_l, out_r, img = s["in_l"], s["in_r"], s["out_l"], s["out_r"], s["img"]
    right, basis_own, load = s["right"], s["basis_own"], s["load"]
    basis_hl, sc, sc_hl = s["basis_hl"], s["sc"], s["sc_hl"]
    p_ref, z, base, zbase, si = s["p"], s["z"], s["base"], s["zbase"], s["si"]
    lam, amp_out, d = s["lam"], s["amp"], s["d"]
    m_ref, sweep = s["m"], s["sweep"]
    scal_in, scal_mid, scal_x, scal_y = s["scal_in"], s["scal_mid"], s["scal_x"], s["scal_y"]

    def where_is(i):
        return (lax.div(i, ny), lax.rem(i, ny))

    def fetch(i, slot):
        return pltpu.make_async_copy(
            schur_ref.at[pl.ds(i * GROUP, GROUP), :], stages[slot], s["stage_sem"].at[slot]
        )

    def load_in(k):
        src, dst = ((basis_hbm, basis_own), (right_hbm, right), (load_hbm, load))[k]
        return pltpu.make_async_copy(src, dst, s["load_sem"].at[k])

    load_in(0).start()
    barrier = pltpu.get_barrier_semaphore()

    def greet(x, y):
        pl.semaphore_signal(barrier, inc=1, device_id=(x, y), device_id_type=MESH)

    def greet_x(k, carry):
        greet(lax.rem(ix + k, nx), iy)
        return carry

    def greet_y(k, carry):
        greet(ix, lax.rem(iy + k, ny))
        return carry

    turns_left = jnp.logical_and(iy == 0, ix > 0)
    turns_right = jnp.logical_and(iy == ny - 1, ix < nx - 1)

    lax.fori_loop(1, nx, greet_x, 0)
    lax.fori_loop(1, ny, greet_y, 0)

    @pl.when(turns_left)
    def _():
        greet(ix - 1, ny - 1)

    @pl.when(turns_right)
    def _():
        greet(ix + 1, 0)

    load_in(1).start()
    for i in range(SLOTS):
        fetch(i, i).start()
    load_in(2).start()

    @pl.when(me == 0)
    def _():
        in_l[...] = jnp.zeros_like(in_l)

    @pl.when(me == n - 1)
    def _():
        in_r[...] = jnp.zeros_like(in_r)

    def to_right(e, i, src):
        return pltpu.make_async_remote_copy(
            src_ref=src, dst_ref=in_l.at[e, pl.ds(i * low, low)], send_sem=s["hs_r"].at[e, i],
            recv_sem=s["hr_l"].at[e, i], device_id=where_is(lax.rem(me + 1, n)), device_id_type=MESH,
        )

    def to_left(e, i, src):
        return pltpu.make_async_remote_copy(
            src_ref=src, dst_ref=in_r.at[e, pl.ds(i * low, low)], send_sem=s["hs_l"].at[e, i],
            recv_sem=s["hr_r"].at[e, i], device_id=where_is(lax.rem(me + n - 1, n)), device_id_type=MESH,
        )

    any_part = out_l.at[0, pl.ds(0, low)]

    def send(e, i_right, src_right, i_left, src_left):
        if src_left is not None:
            @pl.when(me > 0)
            def _():
                to_left(e, i_left, src_left).start()

        if src_right is not None:
            @pl.when(me < n - 1)
            def _():
                to_right(e, i_right, src_right).start()

    def from_left(e, i):
        @pl.when(me > 0)
        def _():
            to_right(e, i, any_part).wait_recv()

        return in_l[e, i * low : (i + 1) * low, :]

    def from_right(e, i):
        @pl.when(me < n - 1)
        def _():
            to_left(e, i, any_part).wait_recv()

        return in_r[e, i * low : (i + 1) * low, :]

    def below(c):
        return lax.broadcasted_iota(jnp.int32, (low, nc), 0) + c * low < off

    def q(c):
        return slice(c * low, (c + 1) * low)

    def own_q(c):
        return slice(slab + c * low, slab + (c + 1) * low)

    def send_own(e, c, ref):
        view = ref.at[pl.ds(c * low, low)]
        send(e, c - 1, view if c > 0 else None, c, view if c < 3 else None)

    def halo(e, c):
        if c == 0:
            return from_right(e, 0)
        if c == 3:
            return from_left(e, 2)
        left = from_left(e, c - 1)
        return jnp.where(below(c), from_right(e, c), left)

    def send_parts(e, k, c, head):
        mask = below(c)
        if c < 3:
            out_r[k, q(c), :] = jnp.where(mask, head, 0.0) if c > 0 else head
        if c > 0:
            out_l[k, q(c - 1), :] = jnp.where(mask, 0.0, head) if c < 3 else head
        send(
            e,
            c, out_r.at[k, pl.ds(c * low, low)] if c < 3 else None,
            c - 1, out_l.at[k, pl.ds((c - 1) * low, low)] if c > 0 else None,
        )

    def add_parts(e, c, mine):
        if c < 3:
            mine = mine + from_left(e, c)
        if c > 0:
            mine = mine + from_right(e, c - 1)
        return mine

    def put(rows, value):
        hi, lo = halves(value)
        vec[rows, :nc] = hi
        vec[rows, nc:] = lo

    def product(at, pieces):
        total = None
        for k0, k1 in pieces:
            both = jnp.dot(s_hi[at, k0:k1], vec[k0:k1, :], preferred_element_type=F32)
            rest = jnp.dot(s_lo[at, k0:k1], vec[k0:k1, :nc], preferred_element_type=F32)
            part = both[:, :nc] + (both[:, nc:] + rest)
            total = part if total is None else total + part
        return total

    def mul(pieces, first=False, last=False):
        tall = width if not first else slab

        def rows(i, carry):
            at = pl.ds(pl.multiple_of(i * tall, tall), tall)
            acc = product(at, pieces)
            if not first:
                acc = twice[at, :] + acc
            twice[at, :] = acc
            if last:
                twice[pl.ds(pl.multiple_of(width + i * tall, tall), tall), :] = acc
            return carry

        lax.fori_loop(0, width // tall, rows, 0)

    def mul_quarters(cs, last=False):
        mul([(c * low, (c + 1) * low) for c in cs], last=last)

    def folded(first, count):
        return twice[pl.ds(width - off + first, count), :]

    def x_send(src, dst, sends, recvs):
        for k in range(1, nx):
            peer = lax.rem(ix + k, nx)
            pltpu.make_async_remote_copy(
                src_ref=src(peer), dst_ref=dst, send_sem=sends, recv_sem=recvs,
                device_id=(peer, iy), device_id_type=MESH,
            ).start()

    def y_send(src, dst, sends, recvs):
        def go(k, carry):
            peer = lax.rem(iy + k, ny)
            pltpu.make_async_remote_copy(
                src_ref=src(peer), dst_ref=dst, send_sem=sends, recv_sem=recvs,
                device_id=(ix, peer), device_id_type=MESH,
            ).start()
            return carry

        lax.fori_loop(1, ny, go, 0)

    def wait_for(ref, count, sem):
        view = ref.at[pl.ds(0, count)]
        pltpu.make_async_copy(view, view, sem).wait()

    def red(r):
        return [s[name + str(r)] for name in ("pa", "fa", "pb", "fb", "ga", "gb")]

    def red1(r, value):
        pa, fa = red(r)[:2]
        h = value.shape[0] // nx
        for i in range(nx):
            pa[i] = value[i * h : (i + 1) * h]
        x_send(lambda peer: pa.at[peer], fa.at[ix], s["rs"].at[r, 0], s["rr"].at[r, 0])
        fa[ix] = pa[ix]

    def red2(r):
        _, fa, pb, fb = red(r)[:4]
        wait_for(fa, nx - 1, s["rr"].at[r, 0])
        total = jnp.sum(fa[...], axis=0)
        h = total.shape[0] // ny
        for i in range(ny):
            pb[i] = total[i * h : (i + 1) * h]
        y_send(lambda peer: pb.at[peer], fb.at[iy], s["rs"].at[r, 1], s["rr"].at[r, 1])
        fb[iy] = pb[iy]

    def red3(r):
        fb, ga = red(r)[3:5]
        wait_for(fb, ny - 1, s["rr"].at[r, 1])
        ga[iy] = jnp.sum(fb[...], axis=0)
        y_send(lambda peer: ga.at[iy], ga.at[iy], s["rs"].at[r, 2], s["rr"].at[r, 2])

    def red4(r):
        ga, gb = red(r)[4:]
        wait_for(ga, ny - 1, s["rr"].at[r, 2])
        x_send(lambda peer: ga, gb.at[ix], s["rs"].at[r, 3], s["rr"].at[r, 3])
        gb[ix] = ga[...]

    def red5(r):
        gb = red(r)[5]
        wait_for(gb, nx - 1, s["rr"].at[r, 3])
        h = gb.shape[2]
        for i in range(nx):
            for j in range(ny):
                m_ref[(i * ny + j) * h : (i * ny + j + 1) * h, :] = gb[i, j]
        return m_ref[: n * h, :]

    def scal1(it):
        y_send(lambda peer: scal_in.at[it], scal_y.at[it, iy], s["ss"].at[it, 1], s["sr"].at[it, 1])
        scal_y[it, iy] = scal_in[it]

    def scal2(it):
        wait_for(scal_y.at[it], ny - 1, s["sr"].at[it, 1])
        scal_mid[it] = jnp.sum(scal_y[it], axis=0)
        x_send(lambda peer: scal_mid.at[it], scal_x.at[it, ix], s["ss"].at[it, 0], s["sr"].at[it, 0])
        scal_x[it, ix] = scal_mid[it]

    def scal3(it):
        wait_for(scal_x.at[it], nx - 1, s["sr"].at[it, 0])
        sums = jnp.sum(scal_x[it], axis=0)
        return sums[0:1], sums[1:2], sums[2:3]

    def scal_all(it):
        all_send(lambda peer: scal_in.at[it], s["scal_a"].at[me], s["ss"].at[it, 0], s["sr"].at[it, 0])
        s["scal_a"][me] = scal_in[it]

    def scal_sum(it):
        wait_for(s["scal_a"], n - 1, s["sr"].at[it, 0])
        sums = jnp.sum(s["scal_a"][...], axis=0)
        return sums[0:1], sums[1:2], sums[2:3]

    def all_send(src, dst, sends, recvs):
        def go(k, carry):
            peer = lax.rem(me + k, n)
            pltpu.make_async_remote_copy(
                src_ref=src(peer), dst_ref=dst, send_sem=sends, recv_sem=recvs,
                device_id=where_is(peer), device_id_type=MESH,
            ).start()
            return carry

        lax.fori_loop(1, n, go, 0)

    def direct1(value):
        h = value.shape[0] // n
        for i in range(n):
            s["dp"][i] = value[i * h : (i + 1) * h]
        all_send(lambda peer: s["dp"].at[peer], s["df"].at[me], s["ds"].at[0], s["dr"].at[0])
        s["df"][me] = s["dp"][me]

    def direct2():
        wait_for(s["df"], n - 1, s["dr"].at[0])
        s["dt"][me] = jnp.sum(s["df"][...], axis=0)
        all_send(lambda peer: s["dt"].at[me], s["dt"].at[me], s["ds"].at[1], s["dr"].at[1])

    def direct3():
        wait_for(s["dt"], n - 1, s["dr"].at[1])
        h = s["dt"].shape[1]
        for i in range(n):
            m_ref[i * h : (i + 1) * h, :] = s["dt"][i]
        return m_ref[: n * h, :]

    turn, twist = lax.div(off, LANES), lax.rem(off, LANES)
    wraps = lax.broadcasted_iota(jnp.int32, (CHUNK, LANES), 1) < twist

    def split(g):
        slot = g % SLOTS
        fetch(g, slot).wait()
        for i in range(GROUP // CHUNK):
            rows = slice(i * CHUNK, (i + 1) * CHUNK)
            at = slice(g * GROUP + i * CHUNK, g * GROUP + (i + 1) * CHUNK)

            def rolled(j):
                m = lax.rem(j - turn + tiles, tiles) * LANES
                return pltpu.roll(stages[slot][rows, pl.ds(m, LANES)], twist, 1)

            before = rolled(-1)
            for j in range(tiles):
                now = rolled(j)
                hi, lo = halves(jnp.where(wraps, before, now))
                s_hi[at, j * LANES : (j + 1) * LANES] = hi
                s_lo[at, j * LANES : (j + 1) * LANES] = lo
                before = now
        if g + SLOTS < groups:
            fetch(g + SLOTS, slot).start()

    def mul_group(g):
        at = slice(g * GROUP, (g + 1) * GROUP)
        twice[at, :] = product(at, [(slab, width)])

    load_in(0).wait()
    load_in(1).wait()
    own_t = basis_own[...].T
    both = dot(own_t, jnp.concatenate([basis_own[...], right[...]], axis=1))
    m_ref[nc:, :] = both[:, nc:]
    hi, lo = halves(own_t)
    s["bt_hi"][:, slab:] = hi
    s["bt_lo"][:, slab:] = lo
    put(slice(slab, width), basis_own[...])
    corners = jnp.where(turns_left, 1, 0) + jnp.where(turns_right, 1, 0)
    pl.semaphore_wait(barrier, nx + ny - 2 + corners)

    red1(0, both[:, :nc])
    send_own(0, 1, basis_own)
    split(0)
    mul_group(0)
    split(1)
    red2(0)
    for c in STEPS[1]:
        send_own(0, c, basis_own)
    for g in range(2, groups):
        mul_group(g - 1)
        split(g)
    red3(0)
    for c in STEPS[2]:
        send_own(0, c, basis_own)
    mul_group(groups - 1)
    for step, cs in enumerate(STEPS):
        for c in cs:
            value = halo(0, c)
            hi, lo = halves(value.T)
            s["bt_hi"][:, q(c)] = hi
            s["bt_lo"][:, q(c)] = lo
            put(q(c), value)
        mul_quarters(cs, last=step == 2)
        if step == 1:
            red4(0)
    basis_hl[...] = vec[...]

    for cs in STEPS[:2]:
        for c in cs:
            head = folded(c * low, low)
            send_parts(1, 0, c, head)
            sc[q(c), :] = head
    for c in STEPS[2]:
        sc[q(c), :] = folded(c * low, low)
    sc[slab:, :] = folded(slab, slab)
    sc_hl[...] = narrow(sc[...])
    both = jnp.dot(s["bt_hi"][...], sc_hl[...], preferred_element_type=F32)
    rest = jnp.dot(s["bt_lo"][...], sc_hl[:, :nc], preferred_element_type=F32)
    red1(1, jnp.concatenate([both[:, :nc] + (both[:, nc:] + rest), m_ref[nc:, :]], axis=0))
    sweep[...] = red5(0)

    lanes = lax.broadcasted_iota(jnp.int32, (nc, nc), 1)
    subs = lax.broadcasted_iota(jnp.int32, (nc, nc), 0)

    def eliminate(a, k, row, col, p):
        here = lanes == k
        inverse = 1.0 / p
        scaled = row * inverse
        new = a - col * scaled
        new = jnp.where(here, col * inverse, new)
        return jnp.where(subs == k, jnp.where(here, -inverse, scaled), new), scaled, inverse

    def pick(row, k):
        return jnp.sum(jnp.where(lanes[:1] == k, row, 0.0), axis=1, keepdims=True)

    def pivot(turn, a):
        k = PIVOTS * turn
        some = range(PIVOTS)
        rows = [sweep[pl.ds(k + i, 1), :] for i in some]
        cols = [jnp.sum(jnp.where(lanes == k + i, a, 0.0), axis=1, keepdims=True) for i in some]
        block = {(i, j): pick(rows[i], k + j) for i in some for j in some if i <= j}
        for i in some:
            a, scaled, inverse = eliminate(a, k + i, rows[i], cols[i], block[i, i])
            for j in range(i + 1, PIVOTS):
                ratio = block[i, j] * inverse
                rows[j] = jnp.where(lanes[:1] == k + i, ratio, rows[j] - block[i, j] * scaled)
                cols[j] = jnp.where(subs[:, :1] == k + i, ratio, cols[j] - cols[i] * ratio)
                for l in range(j, PIVOTS):
                    block[j, l] = block[j, l] - ratio * block[i, l]
        sweep[...] = a
        return a

    half_way = lax.fori_loop(0, nc // PIVOTS // 2, pivot, sweep[...])
    red2(1)
    for c in STEPS[2]:
        send_parts(1, 0, c, sc[q(c), :])
    ginv = -lax.fori_loop(nc // PIVOTS // 2, nc // PIVOTS, pivot, half_way)
    load_in(2).wait()
    y0 = dot(ginv, load[...])
    y0_op = right_operand(y0)

    fc = s["fc"]
    for cs in STEPS:
        for c in cs:
            fc_c = add_parts(1, c, sc[own_q(c), :])
            fc[q(c), :] = fc_c
            img[0, own_q(c), :] = right[q(c), :] - small(narrow(fc_c), y0_op)
            send_own(2, c, img.at[0, pl.ds(slab, slab)])
        if cs == STEPS[0]:
            red3(1)
    fc_hi, fc_lo = halves(fc[...].T)
    s["fct_hi"][...] = fc_hi
    s["fct_lo"][...] = fc_lo

    def coarse(rows):
        both = jnp.dot(s["fct_hi"][...], rows, preferred_element_type=F32)
        rest = jnp.dot(s["fct_lo"][...], rows[:, :nc], preferred_element_type=F32)
        return both[:, :nc] + (both[:, nc:] + rest)

    red1(2, coarse(narrow(img[0, slab:, :])))
    put(slice(slab, width), img[0, slab:, :])
    mul([(slab, width)], first=True)
    red4(1)
    red2(2)
    lam[...] = small(basis_hl[slab:, :], y0_op)

    def own_z(op, step, beta, old):
        cs = small(basis_hl[slab:, :], op)
        if step is None:
            z[slab:, :] = img[old, slab:, :] - cs
        elif beta is None:
            z[slab:, :] = z[slab:, :] + step * (cs - img[old + 1, slab:, :])
        else:
            z[slab:, :] = z[slab:, :] + step * (cs - beta * img[old, slab:, :] - img[old + 1, slab:, :])

    def bases(op, step, beta, old):
        def rows(i, carry):
            at = pl.ds(pl.multiple_of(i * BLOCK, BLOCK), BLOCK)
            ss = small(sc_hl[at, :], op)
            if step is None:
                base[at, :] = -ss
            elif beta is None:
                base[at, :] = p_ref[at, :] + step * ss
            else:
                base[at, :] = p_ref[at, :] + step * (ss - beta * si[at, :])
            return carry

        def halo_rows(i, carry):
            at = pl.ds(pl.multiple_of(i * BLOCK, BLOCK), BLOCK)
            cs = small(basis_hl[at, :], op)
            if step is None:
                zbase[at, :] = -cs
            elif beta is None:
                zbase[at, :] = z[at, :] + step * cs
            else:
                zbase[at, :] = z[at, :] + step * (cs - beta * img[old, at, :])
            return carry

        lax.fori_loop(0, width // BLOCK, rows, 0)
        lax.fori_loop(0, slab // BLOCK, halo_rows, 0)

    def own_scalars(it, beta):
        mine = z[slab:, :]
        scal_in[it, 1:2] = jnp.sum(mine * mine, axis=0, keepdims=True)
        scal_in[it, 3:4] = jnp.zeros((1, nc), F32)
        if it == 0:
            scal_in[it, 2:3] = jnp.zeros((1, nc), F32)
            return
        image = img[it, slab:, :]
        if it > 1:
            image = image + beta * s["image"][...]
        s["image"][...] = image
        scal_in[it, 2:3] = jnp.sum(mine * image, axis=0, keepdims=True)

    energy = curvature = coarse_image = step = beta = None
    for it in range(ITERS):
        last = it == ITERS - 1
        e = 2 + 2 * it
        scale = 1.0 if it == 0 else -step
        r = 2 + it

        for k, cs in enumerate(STEPS):
            for c in cs:
                value = halo(e, c)
                img[it, q(c), :] = value
                put(q(c), value)
            mul_quarters(cs, last=k == 2)
            if k == 0 and it == 0:
                sums = red5(1)
                cfc = s["cfc"]
                cfc[...] = sums[:nc]
                amp = dot(ginv, sums[nc:] - dot(cfc[...], y0))
                known = -dot(cfc[...], amp)
                op = right_operand(amp)
                own_z(op, None, None, 0)
                own_scalars(0, None)
                bases(op, None, None, 0)

        def next_p(c):
            p_c = base[q(c), :] + scale * folded(c * low, low)
            p_ref[q(c), :] = p_c
            if not last:
                send_parts(e + 1, 1 + it, c, p_c)

        for c in STEPS[0]:
            next_p(c)
        for c in STEPS[1] + STEPS[2]:
            p_ref[q(c), :] = base[q(c), :] + scale * folded(c * low, low)
        p_ref[slab:, :] = base[slab:, :] + scale * folded(slab, slab)
        z[:slab, :] = zbase[:slab, :] + scale * img[it, :slab, :]
        scal_in[it, 0:1] = jnp.sum(z[...] * p_ref[...], axis=0, keepdims=True)
        if last:
            scal_all(it)
            direct2()
        else:
            scal1(it)
        if not last:
            red3(r)
            for c in STEPS[1] + STEPS[2]:
                send_parts(e + 1, 1 + it, c, p_ref[q(c), :])
        if it > 0 and not last:
            raw = folded(0, width)
            si[...] = raw if it == 1 else raw + beta * si[...]

        def next_image(cs):
            for c in cs:
                value = add_parts(e + 1, c, p_ref[own_q(c), :])
                img[it + 1, own_q(c), :] = value
                send_own(e + 2, c, img.at[it + 1, pl.ds(slab, slab)])
                put(own_q(c), value)

        def mul_own(cs):
            mul([(slab + c * low, slab + (c + 1) * low) for c in cs], first=cs == STEPS[0])

        if not last:
            next_image(STEPS[0])
            mul_own(STEPS[0])
        if not last:
            scal2(it)
            red4(r)
        if not last:
            next_image(STEPS[1])
            mul_own(STEPS[1])
            next_image(STEPS[2])
            local = coarse(narrow(img[it + 1, slab:, :]))
            if it + 1 < ITERS - 1:
                red1(r + 1, local)
            else:
                direct1(local)
            mul_own(STEPS[2])
        curved, energy_now, crossed = scal_sum(it) if last else scal3(it)
        raw_coarse = direct3() if last else red5(r)
        if it == 0:
            coarse_z = known + raw_coarse
            coarse_image = coarse_z
            d[...] = z[slab:, :]
            curvature = curved
        else:
            images = raw_coarse if it == 1 else raw_coarse + beta * images
            coarse_z = known - step * images
            beta = energy_now / energy
            d[...] = z[slab:, :] + beta * d[...]
            curvature = curved + beta * (2.0 * crossed + beta * curvature)
            coarse_image = coarse_z + beta * coarse_image
        energy = energy_now
        step = energy / curvature
        lam[...] += step * d[...]
        shift = dot(ginv, coarse_image)
        amp = amp - step * shift
        if not last:
            op = right_operand(shift)
            own_z(op, step, beta, it)
            own_scalars(it + 1, beta)
            if it + 1 < ITERS - 1:
                red2(r + 1)
            bases(op, step, beta, it)
            known = coarse_z + step * dot(cfc[...], shift)

    amp_out[...] = amp
    out_lam = pltpu.make_async_copy(lam, lam_hbm, s["load_sem"].at[0])
    out_amp = pltpu.make_async_copy(amp_out, amp_hbm, s["load_sem"].at[1])
    out_lam.start()
    out_amp.start()

    for e in range(EXCHANGES):
        for i in range(3):
            @pl.when(me > 0)
            def _():
                to_left(e, i, any_part).wait_send()

            @pl.when(me < n - 1)
            def _():
                to_right(e, i, any_part).wait_send()

    for r in range(REDUCES):
        pa, _, pb, _, ga, gb = red(r)
        wait_for(pa, nx - 1, s["rs"].at[r, 0])
        wait_for(pb, ny - 1, s["rs"].at[r, 1])
        wait_for(ga, ny - 1, s["rs"].at[r, 2])
        wait_for(gb, nx - 1, s["rs"].at[r, 3])
    wait_for(s["scal_a"], n - 1, s["ss"].at[ITERS - 1, 0])
    wait_for(s["dp"], n - 1, s["ds"].at[0])
    wait_for(s["dt"], n - 1, s["ds"].at[1])
    for it in range(ITERS - 1):
        wait_for(scal_x.at[it], nx - 1, s["ss"].at[it, 0])
        wait_for(scal_y.at[it], ny - 1, s["ss"].at[it, 1])
    out_lam.wait()
    out_amp.wait()


def finish(lam_in, amp_in, lam_out, amp_out, lam, amp, sems):
    arrive = [
        pltpu.make_async_copy(lam_in, lam, sems.at[0]),
        pltpu.make_async_copy(amp_in, amp, sems.at[1]),
    ]
    leave = [
        pltpu.make_async_copy(lam, lam_out, sems.at[2]),
        pltpu.make_async_copy(amp, amp_out, sems.at[3]),
    ]
    for copy in arrive:
        copy.start()
    for there, back in zip(arrive, leave):
        there.wait()
        back.start()
    for copy in leave:
        copy.wait()


def entry(nx, ny, names, *refs):
    fixed = len(refs) - len(names)
    kernel(nx, ny, *refs[:fixed], dict(zip(names, refs[fixed:])))


def solution(mesh):
    nx, ny = mesh.shape["gx"], mesh.shape["gy"]

    def local(schur_blocks, offsets, right_side, coarse_basis, coarse_load):
        slab, r = right_side.shape
        nc = coarse_basis.shape[1]
        width = schur_blocks.shape[1]
        span = slab - slab // 4
        vmem, dma = pltpu.VMEM, pltpu.SemaphoreType.DMA
        scratch = {"stage%d" % i: vmem((GROUP, width), F32) for i in range(SLOTS)}
        scratch |= {name: vmem((width, width), BF16) for name in ("s_hi", "s_lo")}
        scratch |= {name: vmem((width, 2 * nc), BF16) for name in ("vec", "basis_hl", "sc_hl")}
        scratch |= {name: vmem((width, r), F32) for name in ("sc", "p", "z", "base", "zbase", "si")}
        scratch |= {name: vmem((slab, r), F32) for name in ("right", "basis_own", "lam", "d", "fc", "image")}
        scratch |= {name: vmem((nc, r), F32) for name in ("load", "amp", "sweep", "cfc")}
        scratch |= {name: vmem((nc, slab), BF16) for name in ("fct_hi", "fct_lo")}
        scratch |= {name: vmem((nc, width), BF16) for name in ("bt_hi", "bt_lo")}
        scratch |= {
            "twice": vmem((2 * width, r), F32),
            "img": vmem((IMAGES, width, r), F32),
            "out_l": vmem((PARTS, span, r), F32),
            "out_r": vmem((PARTS, span, r), F32),
            "in_l": vmem((EXCHANGES, span, r), F32),
            "in_r": vmem((EXCHANGES, span, r), F32),
            "m": vmem((2 * nc, r), F32),
            "scal_in": vmem((ITERS, 4, r), F32),
            "scal_mid": vmem((ITERS, 4, r), F32),
            "scal_a": vmem((nx * ny, 4, r), F32),
            "scal_x": vmem((ITERS, nx, 4, r), F32),
            "scal_y": vmem((ITERS, ny, 4, r), F32),
        }
        for k in range(REDUCES):
            rows = 2 * nc if k == 1 else nc
            h, p = rows // nx, rows // (nx * ny)
            scratch |= {
                "pa%d" % k: vmem((nx, h, r), F32),
                "fa%d" % k: vmem((nx, h, r), F32),
                "pb%d" % k: vmem((ny, p, r), F32),
                "fb%d" % k: vmem((ny, p, r), F32),
                "ga%d" % k: vmem((ny, p, r), F32),
                "gb%d" % k: vmem((nx, ny, p, r), F32),
            }
        scratch |= {name: vmem((nx * ny, nc // (nx * ny), r), F32) for name in ("dp", "df", "dt")}
        scratch |= {name: dma((EXCHANGES, 3)) for name in ("hs_l", "hs_r", "hr_l", "hr_r")}
        scratch |= {
            "ds": dma((2,)),
            "dr": dma((2,)),
            "stage_sem": dma((SLOTS,)),
            "load_sem": dma((3,)),
            "rs": dma((REDUCES, 4)),
            "rr": dma((REDUCES, 4)),
            "ss": dma((ITERS, 2)),
            "sr": dma((ITERS, 2)),
        }
        names = tuple(scratch)
        hbm = pl.BlockSpec(memory_space=pl.ANY)
        found = pl.pallas_call(
            functools.partial(entry, nx, ny, names),
            out_shape=(
                jax.ShapeDtypeStruct((slab, r), F32),
                jax.ShapeDtypeStruct((nc, r), F32),
            ),
            in_specs=[pl.BlockSpec(memory_space=pltpu.SMEM), hbm, hbm, hbm, hbm],
            out_specs=(hbm, hbm),
            scratch_shapes=list(scratch.values()),
            compiler_params=pltpu.CompilerParams(
                collective_id=0, has_side_effects=True, vmem_limit_bytes=60 * 1024 * 1024
            ),
            name="projected_cg",
        )(offsets, schur_blocks[0], right_side, coarse_basis, coarse_load)
        return pl.pallas_call(
            finish,
            out_shape=(
                jax.ShapeDtypeStruct((slab, r), F32),
                jax.ShapeDtypeStruct((nc, r), F32),
            ),
            in_specs=[hbm, hbm],
            out_specs=(hbm, hbm),
            scratch_shapes=[vmem((slab, r), F32), vmem((nc, r), F32), dma((4,))],
            compiler_params=pltpu.CompilerParams(vmem_limit_bytes=2 * 1024 * 1024),
            name="finish",
        )(*found)

    in_specs = (
        P(("gx", "gy"), None, None),
        P(("gx", "gy")),
        P(("gx", "gy"), None),
        P(("gx", "gy"), None),
        P(),
    )
    out_specs = (P(("gx", "gy"), None), P())
    return jax.shard_map(local, mesh=mesh, in_specs=in_specs, out_specs=out_specs, check_vma=False)
```
